256 devices in a mesh: blk: 16 (over y_hi, x, core), member: 16 (over z, y_lo).
Axes of the slice: x: 4, y: 4 (y_hi: 2, y_lo: 2; y = y_hi * 2 + y_lo), z: 8, core: 2. Of those that a mesh axis runs over, the one named last changes fastest.
Arguments:
- coords: float32 [16384, 64], P(('blk', 'member')), may hold values from -6 to 6
- codes: int32 [16384, 16, 1024], P('blk', 'member'), may hold values from 0 to 255
- classes: int32 [16384, 16, 1024], P('blk', 'member'), may hold values from 0 to 3
Outputs:
- final_coords: float32 [16384, 64], P(('blk', 'member'))
The draws below stay inside these ranges and needn't reach their ends.
All inputs are finite; a program needn't handle non-finite values.
Results may differ from the reference program's by a relative error of at most 0.0003.
Values sent between devices are 32-bit elements; how exact they have to be, the bound alone decides.
No kernel may reach another device: no remote copies, remote signals or barrier semaphores. Data moves between devices by JAX's collectives and lax.ppermute only.
A program may use at most 64 MiB of HBM per device.

```python
import jax
import jax.numpy as jnp
from jax import lax

D = 64
ROWS_DEV = 64
ITERS = 3
NPTS = 16384
N_BLK = 16
N_MEMBER = 16


def set_ends(values, key, low, largest):
    longest = values.shape.index(max(values.shape))
    spots = []
    for shift in (0, 1):
        where = [jax.random.randint(jax.random.fold_in(key, axis), (), 0, length) for axis, length in enumerate(values.shape)]
        where[longest] = (where[longest] + shift) % values.shape[longest]
        spots.append(tuple(where))
    return values.at[spots[0]].set(low).at[spots[1]].set(largest)


def steps_of(own_key, extent, pieces, smallest, top_value):
    def one(axis_at, parts):
        heights = jax.random.uniform(jax.random.fold_in(jax.random.fold_in(own_key, 6), axis_at), (parts,), jnp.float32, smallest / len(pieces), top_value / len(pieces))
        return jnp.repeat(jnp.exp(heights), extent[axis_at] // parts).reshape((-1,) + (1,) * (len(extent) - axis_at - 1))

    loudness = one(*pieces[0])
    for cut in pieces[1:]:
        loudness = loudness * one(*cut)
    return loudness


def normal_values(stream_key, extent, deviation, limit, split=(), kind=jnp.bfloat16):
    loudness = steps_of(stream_key, extent, split, -0.22, 0.18) if split else 1.0
    values = jax.random.normal(stream_key, extent, jnp.float32) * deviation * loudness
    return jnp.minimum(jnp.maximum(values, -limit), limit).astype(kind)


def setup_inputs(seed: int = 0) -> dict:
    keys = jax.random.split(jax.random.key(seed), 4)
    coords = normal_values(keys[0], (NPTS, D), 1.0, 6.0, ((0, 256),), jnp.float32)
    codes = set_ends(jax.random.randint(keys[1], (NPTS, N_MEMBER, N_BLK * ROWS_DEV), 0, 256), jax.random.fold_in(keys[1], 1), 0, 255).astype(jnp.int32)
    classes = set_ends(jax.random.randint(keys[2], (NPTS, N_MEMBER, N_BLK * ROWS_DEV), 0, 4), jax.random.fold_in(keys[2], 1), 0, 3).astype(jnp.int32)
    return {"coords": coords, "codes": codes, "classes": classes}


code_step = 0.1
epsilon = 1e-06

def reference(coords, codes, classes):
    total = coords.shape[0]
    band_len = ROWS_DEV * N_MEMBER
    code_rows = codes.reshape(total, N_MEMBER, N_BLK, ROWS_DEV).transpose(0, 2, 1, 3).reshape(total, total)
    class_rows = classes.reshape(total, N_MEMBER, N_BLK, ROWS_DEV).transpose(0, 2, 1, 3).reshape(total, total)
    col_ids = jnp.arange(total, dtype=jnp.int32)

    def update(points):
        norms = lax.optimization_barrier(jnp.sum(points * points, axis=1))

        def one_band(index):
            start = (index * band_len).astype(jnp.int32)
            band = lax.dynamic_slice_in_dim(points, start, band_len, 0)
            code_tile = lax.dynamic_slice_in_dim(code_rows, start, band_len, 0)
            class_tile = lax.dynamic_slice_in_dim(class_rows, start, band_len, 0)
            row_ids = start + jnp.arange(band_len, dtype=jnp.int32)
            self_pair = row_ids[:, None] == col_ids[None, :]
            weights = jnp.where(self_pair, jnp.float32(0.0), 1.0 / (1.0 + class_tile.astype(jnp.float32)))
            targeted = weights * (code_tile.astype(jnp.float32) + 1.0) * code_step
            gram = jnp.dot(band, points.T, precision=lax.Precision.HIGHEST)
            dist_sq = lax.optimization_barrier(jnp.sum(band * band, axis=1))[:, None] + norms[None, :] - 2.0 * gram
            dist_sq = jnp.where(self_pair, jnp.float32(1.0), dist_sq)
            ratio = targeted / jnp.sqrt(dist_sq + epsilon)
            numer = jnp.dot(weights - ratio, points, precision=lax.Precision.HIGHEST)
            return (numer + band * lax.optimization_barrier(jnp.sum(ratio, axis=1))[:, None]) / lax.optimization_barrier(jnp.sum(weights, axis=1))[:, None]
        result = lax.map(one_band, jnp.arange(N_BLK, dtype=jnp.int32))
        return result.reshape(total, points.shape[1])
    for step in range(ITERS):
        coords = update(coords)
    return coords
```

```python
import functools

import jax
import jax.numpy as jnp
from jax import lax
from jax.experimental import pallas as pl
from jax.experimental.pallas import tpu as pltpu
from jax.sharding import PartitionSpec as P

ITERS = 3
CODE_STEP = 0.1
EPSILON = 1e-06

D = 64
LANES = 128
F32, BF16 = jnp.float32, jnp.bfloat16
MIB = 1024 * 1024
VMEM = pl.BlockSpec(memory_space=pltpu.VMEM)
SMEM = pl.BlockSpec(memory_space=pltpu.SMEM)


def lanes_of(shape):
    return lax.broadcasted_iota(jnp.int32, shape, len(shape) - 1)


def prepare_kernel(place, codes, classes, weights, targeted, sums):
    band, slab = weights.shape
    per_row = slab // LANES
    blk, mem = place[0], place[1]
    shape = (8, LANES)
    lane = lanes_of(shape)
    sublane = lax.broadcasted_iota(jnp.int32, shape, 0)
    group = lane // 16

    def one_member(member, _):
        tile = jnp.zeros(shape, F32)
        for g in range(D // 8):
            top = pl.multiple_of(member * D + g * 8, 8)
            total = jnp.zeros(shape, F32)
            for c in range(per_row):
                where = pl.ds(top * per_row + c, 8, stride=per_row)
                code = codes[where, :].astype(F32)
                kind = classes[where, :].astype(F32)
                column = lane + c * LANES - blk * D
                own = (sublane + (top - mem * D) == column) & (column >= 0) & (column < D)
                w = jnp.where(own, 0.0, 1.0 / (1.0 + kind))
                cols = slice(c * LANES, (c + 1) * LANES)
                weights[pl.ds(top, 8), cols] = w
                targeted[pl.ds(top, 8), cols] = w * (code + 1.0) * CODE_STEP
                total = total + w
            tile = jnp.where(group == g, jnp.sum(total, axis=1, keepdims=True), tile)
        sums[member] = tile
        return 0

    lax.fori_loop(0, band // D, one_member, 0)


def prepare(place, codes, classes):
    band, slab = codes.shape[0], codes.shape[-1]
    flat = (band * slab // LANES, LANES)
    return pl.pallas_call(
        prepare_kernel,
        out_shape=(
            jax.ShapeDtypeStruct((band, slab), F32),
            jax.ShapeDtypeStruct((band, slab), F32),
            jax.ShapeDtypeStruct((band // D, 8, LANES), F32),
        ),
        in_specs=[SMEM, VMEM, VMEM],
        out_specs=(VMEM, VMEM, VMEM),
        name="prepare",
        compiler_params=pltpu.CompilerParams(vmem_limit_bytes=20 * MIB),
        cost_estimate=pl.CostEstimate(flops=10**7, bytes_accessed=16 * MIB, transcendentals=0),
    )(place, codes.reshape(flat), classes.reshape(flat))


def split3(x):
    a = x.astype(BF16).astype(F32)
    rest = x - a
    b = rest.astype(BF16).astype(F32)
    return a, b, rest - b


def operand(y, lane, column):
    left = lane < D
    hi = y.astype(BF16).astype(F32)
    lo = (y - hi).astype(BF16).astype(F32)
    square = (hi + lo) * (hi + lo)
    hi_other, lo_other = pltpu.roll(hi, D, 1), pltpu.roll(lo, D, 1)
    halves = []
    for half in range(2):
        norm = jnp.sum(jnp.where(left == (half == 0), square, 0.0), axis=1, keepdims=True)
        if column:
            norm = norm + EPSILON
        a, b, c = split3(jnp.broadcast_to(norm, y.shape))
        h = (hi, hi_other)[half]
        if column:
            extra = jnp.where(lane == 69, c, 0.0)
            extra = jnp.where(lane == 68, b, extra)
            extra = jnp.where(lane == 67, a, extra)
            extra = jnp.where(lane < 67, 1.0, extra)
            first = -2.0 * jnp.where(left, h, (lo_other, lo)[half])
            second = jnp.where(left, -2.0 * h, extra)
        else:
            extra = jnp.where(lane < 70, 1.0, 0.0)
            extra = jnp.where(lane == 66, c, extra)
            extra = jnp.where(lane == 65, b, extra)
            extra = jnp.where(lane == 64, a, extra)
            first = jnp.where(left, h, (hi_other, hi)[half])
            second = jnp.where(left, (lo, lo_other)[half], extra)
        halves.append((first.astype(BF16), second.astype(BF16)))
    return halves


def step_kernel(chunk, rows_ref, columns_ref, weights, targeted, sums, out, left_op, right_op):
    members, packed, _ = rows_ref.shape
    lane = lanes_of((packed, LANES))
    left = lane < D
    for m in range(members):
        for ref, dst, column in ((rows_ref, left_op, False), (columns_ref, right_op, True)):
            for half, (first, second) in enumerate(operand(ref[m], lane, column)):
                at = m * D + half * packed
                dst[at : at + packed, :LANES] = first
                dst[at : at + packed, LANES:] = second
    band, slab = weights.shape
    for c in range(band // chunk):
        rows = slice(c * chunk, (c + 1) * chunk)
        a = left_op[rows, :]
        acc = jnp.zeros((chunk, 2 * LANES), F32)
        for n in range(slab // 256):
            cols = slice(n * 256, (n + 1) * 256)
            b = right_op[cols, :]
            dist_sq = lax.dot_general(a, b, (((1,), (1,)), ((), ())), preferred_element_type=F32)
            gap = weights[rows, cols] - targeted[rows, cols] * lax.rsqrt(jnp.maximum(dist_sq, EPSILON))
            hi = gap.astype(BF16)
            lo = (gap - hi.astype(F32)).astype(BF16)
            acc = acc + jnp.dot(hi, b, preferred_element_type=F32)
            acc = acc + jnp.dot(lo, b, preferred_element_type=F32)
        pulled = acc[:, :LANES]
        pulled = -0.5 * (pulled + pltpu.roll(pulled, D, 1))
        total = jnp.broadcast_to(acc[:, LANES + D : LANES + D + 1], (chunk, LANES))
        for k in range(chunk // D):
            m = c * (chunk // D) + k
            y = rows_ref[m]
            lower = slice(k * D, k * D + packed)
            upper = slice(k * D + packed, (k + 1) * D)
            out[m, :packed, :] = jnp.where(left, pulled[lower] - y * total[lower], pulled[upper] - y * total[upper])
    if out.shape[1] > packed:
        out[:, packed:, :] = sums[...]


def step(rows, columns, weights, targeted, sums, with_sums):
    members, packed, _ = rows.shape
    band, slab = weights.shape
    return pl.pallas_call(
        functools.partial(step_kernel, 256),
        out_shape=jax.ShapeDtypeStruct((members, packed + (8 if with_sums else 0), LANES), F32),
        in_specs=[VMEM] * 5,
        out_specs=VMEM,
        scratch_shapes=[pltpu.VMEM((band, 2 * LANES), BF16), pltpu.VMEM((slab, 2 * LANES), BF16)],
        name="step",
        compiler_params=pltpu.CompilerParams(vmem_limit_bytes=16 * MIB),
        cost_estimate=pl.CostEstimate(flops=2 * 10**9, bytes_accessed=9 * MIB, transcendentals=MIB),
    )(rows, columns, weights, targeted, sums)


def sum_of(parts):
    return functools.reduce(jnp.add, [parts[m] for m in range(parts.shape[0])])


def update_kernel(first, last, parts, own, scale, *outs):
    packed = own.shape[0]
    lane = lanes_of((packed, LANES))
    left = lane < D
    if first:
        tile = sum_of(parts.at[:, packed:, :])
        halves = []
        for half in range(2):
            groups = [half * 4 + k for k in range(packed // 8)]
            halves.append(jnp.concatenate([jnp.broadcast_to(tile[:, g * 16 : g * 16 + 1], (8, LANES)) for g in groups], axis=0))
        inverse = 1.0 / jnp.where(left, halves[0], halves[1])
        outs[-1][...] = inverse
    else:
        inverse = scale[...]
    moved = own[...] + sum_of(parts.at[:, :packed, :]) * inverse
    if last:
        outs[0][:packed, :] = moved[:, :D]
        outs[0][packed:, :] = pltpu.roll(moved, D, 1)[:, :D]
    else:
        outs[0][...] = moved


def update(parts, own, scale, first, last):
    packed = own.shape[0]
    shape = jax.ShapeDtypeStruct((2 * packed, D) if last else own.shape, F32)
    outs = (shape, jax.ShapeDtypeStruct(own.shape, F32)) if first else (shape,)
    return pl.pallas_call(
        functools.partial(update_kernel, first, last),
        out_shape=outs,
        in_specs=[VMEM] * 3,
        out_specs=(VMEM,) * len(outs),
        name="update",
        compiler_params=pltpu.CompilerParams(vmem_limit_bytes=4 * MIB),
    )(parts, own, scale)


def exchange(parts, axis):
    return lax.all_to_all(parts, axis, split_axis=0, concat_axis=0, tiled=True)


def to_all(value, axis):
    return exchange(jnp.broadcast_to(value, (lax.axis_size(axis), *value.shape)), axis)


def body(coords, codes, classes):
    packed = coords.shape[0] // 2
    place = jnp.stack([lax.axis_index("blk"), lax.axis_index("member")]).astype(jnp.int32)
    own = jnp.concatenate([coords[:packed], coords[packed:]], axis=1)
    weights, targeted, sums = prepare(place, codes, classes)
    scale = own
    for at in range(ITERS):
        columns = to_all(own, "blk")
        rows = to_all(own, "member")
        parts = step(rows, columns, weights, targeted, sums, at == 0)
        outs = update(exchange(parts, "member"), own, scale, at == 0, at == ITERS - 1)
        own = outs[0]
        if at == 0:
            scale = outs[1]
    return own


def solution(mesh):
    in_specs = (P(("blk", "member"), None), P("blk", "member", None), P("blk", "member", None))
    out_specs = P(("blk", "member"), None)
    return jax.shard_map(body, mesh=mesh, in_specs=in_specs, out_specs=out_specs, check_vma=False)
```

```python
import functools

import jax
import jax.numpy as jnp
from jax import lax
from jax.experimental import pallas as pl
from jax.experimental.pallas import tpu as pltpu
from jax.sharding import PartitionSpec as P


ITERS = 3
CODE_STEP = 0.1
EPSILON = 1e-06

D = 64
LANES = 128
F32, BF16 = jnp.float32, jnp.bfloat16
MIB = 1024 * 1024
CHUNK = 256
VMEM = pl.BlockSpec(memory_space=pltpu.VMEM)
ANY = pl.BlockSpec(memory_space=pl.ANY)
SMEM = pl.BlockSpec(memory_space=pltpu.SMEM)


def lanes_of(shape):
    return lax.broadcasted_iota(jnp.int32, shape, len(shape) - 1)


def prepare_kernel(place, codes, classes, pair, sums, code_buf, class_buf, pair_buf, in_sems, out_sems):
    _, band, slab = pair.shape
    chunks = in_sems.shape[1]
    per_row = slab // LANES
    height = band // chunks
    fetches, stores = [], []
    for k in range(chunks):
        flat = pl.ds(k * height * per_row, height * per_row)
        rows = pl.ds(k * height, height)
        fetches.append([
            pltpu.make_async_copy(ref.at[flat], buf.at[flat], in_sems.at[at, k])
            for at, (ref, buf) in enumerate(((codes, code_buf), (classes, class_buf)))
        ])
        stores.append([pltpu.make_async_copy(pair_buf.at[at, rows], pair.at[at, rows], out_sems.at[at, k]) for at in (0, 1)])
        for copy in fetches[k]:
            copy.start()
    blk, mem = place[0], place[1]
    shape = (8, LANES)
    lane = lanes_of(shape)
    sublane = lax.broadcasted_iota(jnp.int32, shape, 0)
    group = lane // 16

    def one_member(member, _):
        tile = jnp.zeros(shape, F32)
        for g in range(D // 8):
            top = pl.multiple_of(member * D + g * 8, 8)
            total = jnp.zeros(shape, F32)
            for c in range(per_row):
                where = pl.ds(top * per_row + c, 8, stride=per_row)
                code = code_buf[where, :].astype(F32)
                kind = class_buf[where, :].astype(F32)
                column = lane + c * LANES - blk * D
                own = (sublane + (top - mem * D) == column) & (column >= 0) & (column < D)
                w = jnp.where(own, 0.0, 1.0 / (1.0 + kind))
                cols = slice(c * LANES, (c + 1) * LANES)
                pair_buf[0, pl.ds(top, 8), cols] = w
                pair_buf[1, pl.ds(top, 8), cols] = w * (code + 1.0) * CODE_STEP
                total = total + w
            tile = jnp.where(group == g, jnp.sum(total, axis=1, keepdims=True), tile)
        sums[member] = tile
        return 0

    each = height // D
    for k in range(chunks):
        for copy in fetches[k]:
            copy.wait()
        lax.fori_loop(k * each, (k + 1) * each, one_member, 0)
        for copy in stores[k]:
            copy.start()
    for both in stores:
        for copy in both:
            copy.wait()


def prepare(place, codes, classes):
    band, slab = codes.shape[0], codes.shape[-1]
    flat = (band * slab // LANES, LANES)
    return pl.pallas_call(
        prepare_kernel,
        out_shape=(
            jax.ShapeDtypeStruct((2, band, slab), F32),
            jax.ShapeDtypeStruct((band // D, 8, LANES), F32),
        ),
        in_specs=[SMEM, ANY, ANY],
        out_specs=(ANY, VMEM),
        scratch_shapes=[
            pltpu.VMEM(flat, jnp.int32),
            pltpu.VMEM(flat, jnp.int32),
            pltpu.VMEM((2, band, slab), F32),
            pltpu.SemaphoreType.DMA((2, 4)),
            pltpu.SemaphoreType.DMA((2, 4)),
        ],
        name="prepare",
        compiler_params=pltpu.CompilerParams(vmem_limit_bytes=61 * MIB),
        cost_estimate=pl.CostEstimate(flops=10**7, bytes_accessed=16 * MIB, transcendentals=0),
    )(place, codes.reshape(flat), classes.reshape(flat))


def split3(x):
    a = x.astype(BF16).astype(F32)
    rest = x - a
    b = rest.astype(BF16).astype(F32)
    return a, b, rest - b


def operand(y, lane, column):
    left = lane < D
    hi = y.astype(BF16).astype(F32)
    lo = (y - hi).astype(BF16).astype(F32)
    square = (hi + lo) * (hi + lo)
    hi_other, lo_other = pltpu.roll(hi, D, 1), pltpu.roll(lo, D, 1)
    halves = []
    for half in range(2):
        norm = jnp.sum(jnp.where(left == (half == 0), square, 0.0), axis=1, keepdims=True)
        if column:
            norm = norm + EPSILON
        a, b, c = split3(jnp.broadcast_to(norm, y.shape))
        h = (hi, hi_other)[half]
        if column:
            extra = jnp.where(lane == 69, c, 0.0)
            extra = jnp.where(lane == 68, b, extra)
            extra = jnp.where(lane == 67, a, extra)
            extra = jnp.where(lane < 67, 1.0, extra)
            first = -2.0 * jnp.where(left, h, (lo_other, lo)[half])
            second = jnp.where(left, -2.0 * h, extra)
        else:
            extra = jnp.where(lane < 70, 1.0, 0.0)
            extra = jnp.where(lane == 66, c, extra)
            extra = jnp.where(lane == 65, b, extra)
            extra = jnp.where(lane == 64, a, extra)
            first = jnp.where(left, h, (hi_other, hi)[half])
            second = jnp.where(left, (lo, lo_other)[half], extra)
        halves.append((first.astype(BF16), second.astype(BF16)))
    return halves


def step_kernel(chunk, order, place, rows_ref, near_ref, far_ref, pair, *refs):
    *sums, out, left_op, right_op, pair_buf, sems = refs
    members, packed, _ = rows_ref.shape
    _, band, slab = pair.shape
    fetches = []
    for c in range(band // chunk):
        rows = pl.ds(c * chunk, chunk)
        fetches.append([pltpu.make_async_copy(pair.at[at, rows], pair_buf.at[at, rows], sems.at[at, c]) for at in (0, 1)])
        for copy in fetches[c]:
            copy.start()
    lane = lanes_of((packed, LANES))
    left = lane < D
    for j, steps in enumerate(order):
        ref, k = (near_ref, j) if j < len(order) // 2 else (far_ref, j - len(order) // 2)
        for half, (first, second) in enumerate(operand(ref[k], lane, True)):
            at = pl.multiple_of((place[0] ^ steps) * D + half * packed, packed)
            right_op[pl.ds(at, packed), :LANES] = first
            right_op[pl.ds(at, packed), LANES:] = second
    for m in range(members):
        for half, (first, second) in enumerate(operand(rows_ref[m], lane, False)):
            at = m * D + half * packed
            left_op[at : at + packed, :LANES] = first
            left_op[at : at + packed, LANES:] = second
    for c in range(band // chunk):
        rows = slice(c * chunk, (c + 1) * chunk)
        for copy in fetches[c]:
            copy.wait()
        a = left_op[rows, :]
        acc = jnp.zeros((chunk, 2 * LANES), F32)
        for n in range(slab // 256):
            cols = slice(n * 256, (n + 1) * 256)
            b = right_op[cols, :]
            dist_sq = lax.dot_general(a, b, (((1,), (1,)), ((), ())), preferred_element_type=F32)
            gap = pair_buf[0, rows, cols] - pair_buf[1, rows, cols] * lax.rsqrt(jnp.maximum(dist_sq, EPSILON))
            hi = gap.astype(BF16)
            lo = (gap - hi.astype(F32)).astype(BF16)
            acc = acc + jnp.dot(hi, b, preferred_element_type=F32)
            acc = acc + jnp.dot(lo, b, preferred_element_type=F32)
        pulled = acc[:, :LANES]
        pulled = -0.5 * (pulled + pltpu.roll(pulled, D, 1))
        total = jnp.broadcast_to(acc[:, LANES + D : LANES + D + 1], (chunk, LANES))
        for k in range(chunk // D):
            m = c * (chunk // D) + k
            y = rows_ref[m]
            lower = slice(k * D, k * D + packed)
            upper = slice(k * D + packed, (k + 1) * D)
            out[m, :packed, :] = jnp.where(left, pulled[lower] - y * total[lower], pulled[upper] - y * total[upper])
    if sums:
        out[:, packed:, :] = sums[0][...]


def step(place, rows, columns, pair, *sums):
    members, packed, _ = rows.shape
    _, band, slab = pair.shape
    return pl.pallas_call(
        functools.partial(step_kernel, CHUNK, columns[2]),
        out_shape=jax.ShapeDtypeStruct((members, packed + (8 if sums else 0), LANES), F32),
        in_specs=[SMEM] + [VMEM] * 3 + [ANY] + [VMEM] * len(sums),
        out_specs=VMEM,
        scratch_shapes=[
            pltpu.VMEM((band, 2 * LANES), BF16),
            pltpu.VMEM((slab, 2 * LANES), BF16),
            pltpu.VMEM((2, band, slab), F32),
            pltpu.SemaphoreType.DMA((2, band // CHUNK)),
        ],
        name="step",
        compiler_params=pltpu.CompilerParams(vmem_limit_bytes=50 * MIB),
        cost_estimate=pl.CostEstimate(flops=2 * 10**9, bytes_accessed=9 * MIB, transcendentals=MIB),
    )(place, rows, *columns[:2], pair, *sums)


def sum_of(parts):
    return functools.reduce(jnp.add, [parts[m] for m in range(parts.shape[0])])


def update_kernel(first, last, parts, own, scale, *outs):
    packed = own.shape[0]
    lane = lanes_of((packed, LANES))
    left = lane < D
    if first:
        tile = sum_of(parts.at[:, packed:, :])
        halves = []
        for half in range(2):
            groups = [half * 4 + k for k in range(packed // 8)]
            halves.append(jnp.concatenate([jnp.broadcast_to(tile[:, g * 16 : g * 16 + 1], (8, LANES)) for g in groups], axis=0))
        inverse = 1.0 / jnp.where(left, halves[0], halves[1])
        outs[-1][...] = inverse
    else:
        inverse = scale[...]
    moved = own[...] + sum_of(parts.at[:, :packed, :]) * inverse
    if last:
        outs[0][:packed, :] = moved[:, :D]
        outs[0][packed:, :] = pltpu.roll(moved, D, 1)[:, :D]
    else:
        outs[0][...] = moved


def update(parts, own, scale, first, last):
    packed = own.shape[0]
    shape = jax.ShapeDtypeStruct((2 * packed, D) if last else own.shape, F32)
    outs = (shape, jax.ShapeDtypeStruct(own.shape, F32)) if first else (shape,)
    return pl.pallas_call(
        functools.partial(update_kernel, first, last),
        out_shape=outs,
        in_specs=[VMEM] * 3,
        out_specs=(VMEM,) * len(outs),
        name="update",
        compiler_params=pltpu.CompilerParams(vmem_limit_bytes=4 * MIB),
    )(parts, own, scale)


def exchange(parts, axis):
    return lax.all_to_all(parts, axis, split_axis=0, concat_axis=0, tiled=True)


def swapped(value, steps):
    return lax.ppermute(value, "blk", [(at, at ^ steps) for at in range(lax.axis_size("blk"))])


def column_blocks(own):
    block = own[None]
    held = jnp.concatenate([block, swapped(block, 8)])
    near = jnp.concatenate([held, swapped(held, 2), swapped(held, 6), swapped(held, 4)])
    order = [a ^ b for a in (0, 2, 6, 4) for b in (0, 8)]
    return near, swapped(near, 1), order + [a ^ 1 for a in order]


def body(coords, codes, classes):
    packed = coords.shape[0] // 2
    members = lax.axis_size("member")
    place = jnp.stack([lax.axis_index("blk"), lax.axis_index("member")]).astype(jnp.int32)
    own = jnp.concatenate([coords[:packed], coords[packed:]], axis=1)
    pair, sums = prepare(place, codes, classes)
    scale = own
    for at in range(ITERS):
        rows = exchange(jnp.broadcast_to(own, (members, *own.shape)), "member")
        parts = step(place, rows, column_blocks(own), pair, *((sums,) if at == 0 else ()))
        outs = update(exchange(parts, "member"), own, scale, at == 0, at == ITERS - 1)
        own = outs[0]
        if at == 0:
            scale = outs[1]
    return own


def solution(mesh):
    in_specs = (P(("blk", "member"), None), P("blk", "member", None), P("blk", "member", None))
    out_specs = P(("blk", "member"), None)
    return jax.shard_map(body, mesh=mesh, in_specs=in_specs, out_specs=out_specs, check_vma=False)
```

```python
import functools

import jax
import jax.numpy as jnp
from jax import lax
from jax.experimental import pallas as pl
from jax.experimental.pallas import tpu as pltpu
from jax.sharding import PartitionSpec as P


ITERS = 3
CODE_STEP = 0.1
EPSILON = 1e-06

D = 64
LANES = 128
F32, BF16 = jnp.float32, jnp.bfloat16
MIB = 1024 * 1024
CHUNK = 256
STEP_VMEM = 52 * MIB
VMEM = pl.BlockSpec(memory_space=pltpu.VMEM)
ANY = pl.BlockSpec(memory_space=pl.ANY)
SMEM = pl.BlockSpec(memory_space=pltpu.SMEM)


def lanes_of(shape):
    return lax.broadcasted_iota(jnp.int32, shape, len(shape) - 1)


def split3(x):
    a = x.astype(BF16).astype(F32)
    rest = x - a
    b = rest.astype(BF16).astype(F32)
    return a, b, rest - b


def operand(y, lane, column):
    left = lane < D
    hi = y.astype(BF16).astype(F32)
    lo = (y - hi).astype(BF16).astype(F32)
    square = (hi + lo) * (hi + lo)
    hi_other, lo_other = pltpu.roll(hi, D, 1), pltpu.roll(lo, D, 1)
    halves = []
    for half in range(2):
        norm = jnp.sum(jnp.where(left == (half == 0), square, 0.0), axis=1, keepdims=True)
        if column:
            norm = norm + EPSILON
        a, b, c = split3(jnp.broadcast_to(norm, y.shape))
        h = (hi, hi_other)[half]
        if column:
            extra = jnp.where(lane == 69, c, 0.0)
            extra = jnp.where(lane == 68, b, extra)
            extra = jnp.where(lane == 67, a, extra)
            extra = jnp.where(lane < 67, 1.0, extra)
            first = -2.0 * jnp.where(left, h, (lo_other, lo)[half])
            second = jnp.where(left, -2.0 * h, extra)
        else:
            extra = jnp.where(lane < 70, 1.0, 0.0)
            extra = jnp.where(lane == 66, c, extra)
            extra = jnp.where(lane == 65, b, extra)
            extra = jnp.where(lane == 64, a, extra)
            first = jnp.where(left, h, (hi_other, hi)[half])
            second = jnp.where(left, (lo, lo_other)[half], extra)
        halves.append((first.astype(BF16), second.astype(BF16)))
    return halves


def convert(place, rows, code_buf, class_buf, pair_buf):
    slab = pair_buf.shape[2]
    per_row = slab // LANES

    def sixteen(k, _):
        top = pl.multiple_of(rows[0] + k * 16, 16)
        for c in range(per_row):
            weight, code = [], []
            for g in (0, 8):
                where = pl.ds((top + g) * per_row + c, 8, stride=per_row)
                kind = class_buf[where, :]
                w = jnp.where(kind == 0, 12.0, jnp.where(kind == 1, 6.0, jnp.where(kind == 2, 4.0, 3.0)))
                weight.append(w)
                code.append((code_buf[where, :] + 1).astype(F32))
            cols = slice(c * LANES, (c + 1) * LANES)
            pair_buf[0, pl.ds(top, 16), cols] = jnp.concatenate(weight, axis=0).astype(BF16)
            pair_buf[1, pl.ds(top, 16), cols] = jnp.concatenate(code, axis=0).astype(BF16)
        return 0

    lax.fori_loop(0, (rows[1] - rows[0]) // 16, sixteen, 0)

    @pl.when((place[1] * D >= rows[0]) & (place[1] * D < rows[1]))
    def _():
        top = pl.multiple_of(place[1] * D, D)
        side = pl.multiple_of(place[0] // 2 * LANES, LANES)
        shape = (D, LANES)
        own = lax.broadcasted_iota(jnp.int32, shape, 0) == lanes_of(shape) - place[0] % 2 * D
        w = pair_buf[0, pl.ds(top, D), pl.ds(side, LANES)].astype(F32)
        pair_buf[0, pl.ds(top, D), pl.ds(side, LANES)] = jnp.where(own, 0.0, w).astype(BF16)


def step_kernel(first, order, place, rows_ref, near_ref, far_ref, *refs):
    if first:
        codes, classes, out, pair, left_op, right_op, code_buf, class_buf, pair_buf, in_sems, out_sems = refs
    else:
        pair, out, left_op, right_op, pair_buf, in_sems = refs
    members, packed, _ = rows_ref.shape
    _, band, slab = pair_buf.shape
    per_row = slab // LANES
    chunks = band // CHUNK
    fetches, stores = [], []
    for c in range(chunks):
        rows = pl.ds(c * CHUNK, CHUNK)
        flat = pl.ds(c * CHUNK * per_row, CHUNK * per_row)
        if first:
            fetches.append([
                pltpu.make_async_copy(ref.at[flat], buf.at[flat], in_sems.at[at, c])
                for at, (ref, buf) in enumerate(((codes, code_buf), (classes, class_buf)))
            ])
            stores.append([pltpu.make_async_copy(pair_buf.at[at, rows], pair.at[at, rows], out_sems.at[at, c]) for at in (0, 1)])
        else:
            fetches.append([pltpu.make_async_copy(pair.at[at, rows], pair_buf.at[at, rows], in_sems.at[at, c]) for at in (0, 1)])
    for copy in fetches[0]:
        copy.start()

    lane = lanes_of((packed, LANES))
    left = lane < D
    for j, steps in enumerate(order):
        ref, k = (near_ref, j) if j < len(order) // 2 else (far_ref, j - len(order) // 2)
        for half, (one, two) in enumerate(operand(ref[k], lane, True)):
            at = pl.multiple_of((place[0] ^ steps) * D + half * packed, packed)
            right_op[pl.ds(at, packed), :LANES] = one
            right_op[pl.ds(at, packed), LANES:] = two
    for m in range(members):
        for half, (one, two) in enumerate(operand(rows_ref[m], lane, False)):
            at = m * D + half * packed
            left_op[at : at + packed, :LANES] = one
            left_op[at : at + packed, LANES:] = two

    group = lanes_of((8, LANES)) // 16
    for c in range(chunks):
        rows = slice(c * CHUNK, (c + 1) * CHUNK)
        for copy in fetches[c]:
            copy.wait()
        if c + 1 < chunks:
            for copy in fetches[c + 1]:
                copy.start()
        if first:
            convert(place, (c * CHUNK, (c + 1) * CHUNK), code_buf, class_buf, pair_buf)
            for copy in stores[c]:
                copy.start()
            sums = jnp.dot(pair_buf[0, rows, :], jnp.ones((slab, LANES), BF16), preferred_element_type=F32)
        a = left_op[rows, :]
        acc = jnp.zeros((CHUNK, 2 * LANES), F32)
        for n in range(slab // 256):
            cols = slice(n * 256, (n + 1) * 256)
            b = right_op[cols, :]
            dist_sq = lax.dot_general(a, b, (((1,), (1,)), ((), ())), preferred_element_type=F32)
            near = lax.rsqrt(jnp.maximum(dist_sq, EPSILON)) * CODE_STEP
            weight = pair_buf[0, rows, cols].astype(F32)
            gap = weight - weight * (pair_buf[1, rows, cols].astype(F32) * near)
            hi = gap.astype(BF16)
            lo = (gap - hi.astype(F32)).astype(BF16)
            acc = acc + jnp.dot(hi, b, preferred_element_type=F32)
            acc = acc + jnp.dot(lo, b, preferred_element_type=F32)
        pulled = acc[:, :LANES]
        pulled = -0.5 * (pulled + pltpu.roll(pulled, D, 1))
        total = jnp.broadcast_to(acc[:, LANES + D : LANES + D + 1], (CHUNK, LANES))
        for k in range(CHUNK // D):
            m = c * (CHUNK // D) + k
            y = rows_ref[m]
            lower = slice(k * D, k * D + packed)
            upper = slice(k * D + packed, (k + 1) * D)
            out[m, :packed, :] = jnp.where(left, pulled[lower] - y * total[lower], pulled[upper] - y * total[upper])
            if first:
                tile = jnp.zeros((8, LANES), F32)
                for g in range(D // 8):
                    tile = jnp.where(group == g, sums[k * D + g * 8 : k * D + g * 8 + 8], tile)
                out[m, packed:, :] = tile
    for both in stores:
        for copy in both:
            copy.wait()


def step(place, rows, columns, *sources):
    members, packed, _ = rows.shape
    near, far, order = columns
    first = len(sources) == 2
    band = members * 2 * packed
    slab = len(order) * 2 * packed
    pair = (2, band, slab)
    outs = [jax.ShapeDtypeStruct((members, packed + (8 if first else 0), LANES), F32)]
    scratch = [pltpu.VMEM((band, 2 * LANES), BF16), pltpu.VMEM((slab, 2 * LANES), BF16)]
    sems = pltpu.SemaphoreType.DMA((2, band // CHUNK))
    if first:
        flat = (band * slab // LANES, LANES)
        sources = tuple(source.reshape(flat) for source in sources)
        outs.append(jax.ShapeDtypeStruct(pair, BF16))
        scratch += [pltpu.VMEM(flat, jnp.int32), pltpu.VMEM(flat, jnp.int32), pltpu.VMEM(pair, BF16), sems, sems]
    else:
        scratch += [pltpu.VMEM(pair, BF16), sems]
    return pl.pallas_call(
        functools.partial(step_kernel, first, order),
        out_shape=tuple(outs),
        in_specs=[SMEM] + [VMEM] * 3 + [ANY] * len(sources),
        out_specs=(VMEM, ANY) if first else (VMEM,),
        scratch_shapes=scratch,
        name="step",
        compiler_params=pltpu.CompilerParams(vmem_limit_bytes=STEP_VMEM),
        cost_estimate=pl.CostEstimate(flops=2 * 10**9, bytes_accessed=5 * MIB, transcendentals=MIB),
    )(place, rows, near, far, *sources)


def sum_of(parts):
    return functools.reduce(jnp.add, [parts[m] for m in range(parts.shape[0])])


def update_kernel(first, last, parts, own, scale, *outs):
    packed = own.shape[0]
    lane = lanes_of((packed, LANES))
    left = lane < D
    if first:
        tile = sum_of(parts.at[:, packed:, :])
        halves = []
        for half in range(2):
            groups = [half * 4 + k for k in range(packed // 8)]
            halves.append(jnp.concatenate([jnp.broadcast_to(tile[:, g * 16 : g * 16 + 1], (8, LANES)) for g in groups], axis=0))
        inverse = 1.0 / jnp.where(left, halves[0], halves[1])
        outs[-1][...] = inverse
    else:
        inverse = scale[...]
    moved = own[...] + sum_of(parts.at[:, :packed, :]) * inverse
    if last:
        outs[0][:packed, :] = moved[:, :D]
        outs[0][packed:, :] = pltpu.roll(moved, D, 1)[:, :D]
    else:
        outs[0][...] = moved


def update(parts, own, scale, first, last):
    packed = own.shape[0]
    shape = jax.ShapeDtypeStruct((2 * packed, D) if last else own.shape, F32)
    outs = (shape, jax.ShapeDtypeStruct(own.shape, F32)) if first else (shape,)
    return pl.pallas_call(
        functools.partial(update_kernel, first, last),
        out_shape=outs,
        in_specs=[VMEM] * 3,
        out_specs=(VMEM,) * len(outs),
        name="update",
        compiler_params=pltpu.CompilerParams(vmem_limit_bytes=4 * MIB),
    )(parts, own, scale)


def exchange(parts, axis):
    return lax.all_to_all(parts, axis, split_axis=0, concat_axis=0, tiled=True)


def swapped(value, steps):
    return lax.ppermute(value, "blk", [(at, at ^ steps) for at in range(lax.axis_size("blk"))])


def column_blocks(own):
    block = own[None]
    held = jnp.concatenate([block, swapped(block, 8)])
    near = jnp.concatenate([held, swapped(held, 2), swapped(held, 6), swapped(held, 4)])
    order = [a ^ b for a in (0, 2, 6, 4) for b in (0, 8)]
    return near, swapped(near, 1), order + [a ^ 1 for a in order]


def body(coords, codes, classes):
    packed = coords.shape[0] // 2
    members = lax.axis_size("member")
    place = jnp.stack([lax.axis_index("blk"), lax.axis_index("member")]).astype(jnp.int32)
    own = jnp.concatenate([coords[:packed], coords[packed:]], axis=1)
    scale = own
    sources = (codes, classes)
    for at in range(ITERS):
        rows = exchange(jnp.broadcast_to(own, (members, *own.shape)), "member")
        parts, *pair = step(place, rows, column_blocks(own), *sources)
        if at == 0:
            sources = pair
        outs = update(exchange(parts, "member"), own, scale, at == 0, at == ITERS - 1)
        own = outs[0]
        if at == 0:
            scale = outs[1]
    return own


def solution(mesh):
    in_specs = (P(("blk", "member"), None), P("blk", "member", None), P("blk", "member", None))
    out_specs = P(("blk", "member"), None)
    return jax.shard_map(body, mesh=mesh, in_specs=in_specs, out_specs=out_specs, check_vma=False)
```

```python
import functools

import jax
import jax.numpy as jnp
from jax import lax
from jax.experimental import pallas as pl
from jax.experimental.pallas import tpu as pltpu
from jax.sharding import PartitionSpec as P


ITERS = 3
CODE_STEP = 0.1
EPSILON = 1e-06

D = 64
LANES = 128
F32, BF16 = jnp.float32, jnp.bfloat16
MIB = 1024 * 1024
CHUNK = 256
STEP_VMEM = 52 * MIB
VMEM = pl.BlockSpec(memory_space=pltpu.VMEM)
ANY = pl.BlockSpec(memory_space=pl.ANY)
SMEM = pl.BlockSpec(memory_space=pltpu.SMEM)


def lanes_of(shape):
    return lax.broadcasted_iota(jnp.int32, shape, len(shape) - 1)


def split3(x):
    a = x.astype(BF16).astype(F32)
    rest = x - a
    b = rest.astype(BF16).astype(F32)
    return a, b, rest - b


def operand(y, lane, column):
    left = lane < D
    hi = y.astype(BF16).astype(F32)
    lo = (y - hi).astype(BF16).astype(F32)
    square = (hi + lo) * (hi + lo)
    hi_other, lo_other = pltpu.roll(hi, D, 1), pltpu.roll(lo, D, 1)
    halves = []
    for half in range(2):
        norm = jnp.sum(jnp.where(left == (half == 0), square, 0.0), axis=1, keepdims=True)
        if column:
            norm = norm + EPSILON
        a, b, c = split3(jnp.broadcast_to(norm, y.shape))
        h = (hi, hi_other)[half]
        if column:
            extra = jnp.where(lane == 69, c, 0.0)
            extra = jnp.where(lane == 68, b, extra)
            extra = jnp.where(lane == 67, a, extra)
            extra = jnp.where(lane < 67, 1.0, extra)
            first = -2.0 * jnp.where(left, h, (lo_other, lo)[half])
            second = jnp.where(left, -2.0 * h, extra)
        else:
            extra = jnp.where(lane < 70, 1.0, 0.0)
            extra = jnp.where(lane == 66, c, extra)
            extra = jnp.where(lane == 65, b, extra)
            extra = jnp.where(lane == 64, a, extra)
            first = jnp.where(left, h, (hi_other, hi)[half])
            second = jnp.where(left, (lo, lo_other)[half], extra)
        halves.append((first.astype(BF16), second.astype(BF16)))
    return halves


def convert(place, rows, code_buf, class_buf, pair_buf):
    slab = pair_buf.shape[2]
    per_row = slab // LANES

    def sixteen(k, _):
        top = pl.multiple_of(rows[0] + k * 16, 16)
        for c in range(per_row):
            weight, code = [], []
            for g in (0, 8):
                where = pl.ds((top + g) * per_row + c, 8, stride=per_row)
                kind = class_buf[where, :]
                w = jnp.where(kind == 0, 12.0, jnp.where(kind == 1, 6.0, jnp.where(kind == 2, 4.0, 3.0)))
                weight.append(w)
                code.append((code_buf[where, :] + 1).astype(F32))
            cols = slice(c * LANES, (c + 1) * LANES)
            pair_buf[0, pl.ds(top, 16), cols] = jnp.concatenate(weight, axis=0).astype(BF16)
            pair_buf[1, pl.ds(top, 16), cols] = jnp.concatenate(code, axis=0).astype(BF16)
        return 0

    lax.fori_loop(0, (rows[1] - rows[0]) // 16, sixteen, 0)

    @pl.when((place[1] * D >= rows[0]) & (place[1] * D < rows[1]))
    def _():
        top = pl.multiple_of(place[1] * D, D)
        side = pl.multiple_of(place[0] // 2 * LANES, LANES)
        shape = (D, LANES)
        own = lax.broadcasted_iota(jnp.int32, shape, 0) == lanes_of(shape) - place[0] % 2 * D
        w = pair_buf[0, pl.ds(top, D), pl.ds(side, LANES)].astype(F32)
        pair_buf[0, pl.ds(top, D), pl.ds(side, LANES)] = jnp.where(own, 0.0, w).astype(BF16)


def step_kernel(first, order, place, rows_ref, near_ref, far_ref, *refs):
    if first:
        codes, classes, out, pair, left_op, right_op, code_buf, class_buf, pair_buf, in_sems, out_sems = refs
    else:
        pair, out, left_op, right_op, pair_buf, in_sems = refs
    members, packed, _ = rows_ref.shape
    _, band, slab = pair_buf.shape
    per_row = slab // LANES
    chunks = band // CHUNK

    def fetch(c):
        height = CHUNK * per_row if first else CHUNK
        rows = pl.ds(c * height, height)
        if first:
            ends = ((codes.at[rows], code_buf.at[rows]), (classes.at[rows], class_buf.at[rows]))
        else:
            ends = tuple((pair.at[at, rows], pair_buf.at[at, rows]) for at in (0, 1))
        return [pltpu.make_async_copy(src, dst, in_sems.at[at, c]) for at, (src, dst) in enumerate(ends)]

    def store(c):
        rows = pl.ds(c * CHUNK, CHUNK)
        return [pltpu.make_async_copy(pair_buf.at[at, rows], pair.at[at, rows], out_sems.at[at, c]) for at in (0, 1)]

    def start_fetch(c, _):
        for copy in fetch(c):
            copy.start()
        return 0

    lax.fori_loop(0, chunks, start_fetch, 0)

    lane = lanes_of((packed, LANES))
    left = lane < D
    for j, steps in enumerate(order):
        ref, k = (near_ref, j) if j < len(order) // 2 else (far_ref, j - len(order) // 2)
        for half, (one, two) in enumerate(operand(ref[k], lane, True)):
            at = pl.multiple_of((place[0] ^ steps) * D + half * packed, packed)
            right_op[pl.ds(at, packed), :LANES] = one
            right_op[pl.ds(at, packed), LANES:] = two
    for m in range(members):
        for half, (one, two) in enumerate(operand(rows_ref[m], lane, False)):
            at = m * D + half * packed
            left_op[at : at + packed, :LANES] = one
            left_op[at : at + packed, LANES:] = two

    group = lanes_of((8, LANES)) // 16
    for c in range(chunks):
        rows = slice(c * CHUNK, (c + 1) * CHUNK)
        for copy in fetch(c):
            copy.wait()
        if first:
            convert(place, (c * CHUNK, (c + 1) * CHUNK), code_buf, class_buf, pair_buf)
            for copy in store(c):
                copy.start()
            sums = jnp.dot(pair_buf[0, rows, :], jnp.ones((slab, LANES), BF16), preferred_element_type=F32)
        a = left_op[rows, :]
        acc = jnp.zeros((CHUNK, 2 * LANES), F32)
        for n in range(slab // 256):
            cols = slice(n * 256, (n + 1) * 256)
            b = right_op[cols, :]
            dist_sq = lax.dot_general(a, b, (((1,), (1,)), ((), ())), preferred_element_type=F32)
            near = lax.rsqrt(jnp.maximum(dist_sq, EPSILON))
            gap = pair_buf[0, rows, cols].astype(F32) * (1.0 / CODE_STEP - pair_buf[1, rows, cols].astype(F32) * near)
            acc = acc + jnp.dot(gap.astype(BF16), b, preferred_element_type=F32)
        pulled = acc[:, :LANES]
        pulled = -0.5 * (pulled + pltpu.roll(pulled, D, 1))
        total = jnp.broadcast_to(acc[:, LANES + D : LANES + D + 1], (CHUNK, LANES))
        for k in range(CHUNK // D):
            m = c * (CHUNK // D) + k
            y = rows_ref[m]
            lower = slice(k * D, k * D + packed)
            upper = slice(k * D + packed, (k + 1) * D)
            out[m, :packed, :] = jnp.where(left, pulled[lower] - y * total[lower], pulled[upper] - y * total[upper])
            if first:
                tile = jnp.zeros((8, LANES), F32)
                for g in range(D // 8):
                    tile = jnp.where(group == g, sums[k * D + g * 8 : k * D + g * 8 + 8], tile)
                out[m, packed:, :] = tile
    if first:
        for c in range(chunks):
            for copy in store(c):
                copy.wait()


def step(place, rows, columns, *sources):
    members, packed, _ = rows.shape
    near, far, order = columns
    first = len(sources) == 2
    band = members * 2 * packed
    slab = len(order) * 2 * packed
    pair = (2, band, slab)
    outs = [jax.ShapeDtypeStruct((members, packed + (8 if first else 0), LANES), F32)]
    scratch = [pltpu.VMEM((band, 2 * LANES), BF16), pltpu.VMEM((slab, 2 * LANES), BF16)]
    sems = pltpu.SemaphoreType.DMA((2, band // CHUNK))
    if first:
        flat = (band * slab // LANES, LANES)
        sources = tuple(source.reshape(flat) for source in sources)
        outs.append(jax.ShapeDtypeStruct(pair, BF16))
        scratch += [pltpu.VMEM(flat, jnp.int32), pltpu.VMEM(flat, jnp.int32), pltpu.VMEM(pair, BF16), sems, sems]
    else:
        scratch += [pltpu.VMEM(pair, BF16), sems]
    return pl.pallas_call(
        functools.partial(step_kernel, first, order),
        out_shape=tuple(outs),
        in_specs=[SMEM] + [VMEM] * 3 + [ANY] * len(sources),
        out_specs=(VMEM, ANY) if first else (VMEM,),
        scratch_shapes=scratch,
        name="step",
        compiler_params=pltpu.CompilerParams(vmem_limit_bytes=STEP_VMEM),
        cost_estimate=pl.CostEstimate(flops=2 * 10**9, bytes_accessed=5 * MIB, transcendentals=MIB),
    )(place, rows, near, far, *sources)


def sum_of(parts):
    return functools.reduce(jnp.add, [parts[m] for m in range(parts.shape[0])])


def update_kernel(first, last, parts, own, scale, *outs):
    packed = own.shape[0]
    lane = lanes_of((packed, LANES))
    left = lane < D
    if first:
        tile = sum_of(parts.at[:, packed:, :])
        halves = []
        for half in range(2):
            groups = [half * 4 + k for k in range(packed // 8)]
            halves.append(jnp.concatenate([jnp.broadcast_to(tile[:, g * 16 : g * 16 + 1], (8, LANES)) for g in groups], axis=0))
        inverse = CODE_STEP / jnp.where(left, halves[0], halves[1])
        outs[-1][...] = inverse
    else:
        inverse = scale[...]
    moved = own[...] + sum_of(parts.at[:, :packed, :]) * inverse
    if last:
        outs[0][:packed, :] = moved[:, :D]
        outs[0][packed:, :] = pltpu.roll(moved, D, 1)[:, :D]
    else:
        outs[0][...] = moved


def update(parts, own, scale, first, last):
    packed = own.shape[0]
    shape = jax.ShapeDtypeStruct((2 * packed, D) if last else own.shape, F32)
    outs = (shape, jax.ShapeDtypeStruct(own.shape, F32)) if first else (shape,)
    return pl.pallas_call(
        functools.partial(update_kernel, first, last),
        out_shape=outs,
        in_specs=[VMEM] * 3,
        out_specs=(VMEM,) * len(outs),
        name="update",
        compiler_params=pltpu.CompilerParams(vmem_limit_bytes=4 * MIB),
    )(parts, own, scale)


def exchange(parts, axis):
    return lax.all_to_all(parts, axis, split_axis=0, concat_axis=0, tiled=True)


def swapped(value, steps):
    return lax.ppermute(value, "blk", [(at, at ^ steps) for at in range(lax.axis_size("blk"))])


def column_blocks(own):
    block = own[None]
    held = jnp.concatenate([block, swapped(block, 8)])
    near = jnp.concatenate([held, swapped(held, 2), swapped(held, 6), swapped(held, 4)])
    order = [a ^ b for a in (0, 2, 6, 4) for b in (0, 8)]
    return near, swapped(near, 1), order + [a ^ 1 for a in order]


def body(coords, codes, classes):
    packed = coords.shape[0] // 2
    members = lax.axis_size("member")
    place = jnp.stack([lax.axis_index("blk"), lax.axis_index("member")]).astype(jnp.int32)
    own = jnp.concatenate([coords[:packed], coords[packed:]], axis=1)
    scale = own
    sources = (codes, classes)
    for at in range(ITERS):
        rows = exchange(jnp.broadcast_to(own, (members, *own.shape)), "member")
        parts, *pair = step(place, rows, column_blocks(own), *sources)
        if at == 0:
            sources = pair
        outs = update(exchange(parts, "member"), own, scale, at == 0, at == ITERS - 1)
        own = outs[0]
        if at == 0:
            scale = outs[1]
    return own


def solution(mesh):
    in_specs = (P(("blk", "member"), None), P("blk", "member", None), P("blk", "member", None))
    out_specs = P(("blk", "member"), None)
    return jax.shard_map(body, mesh=mesh, in_specs=in_specs, out_specs=out_specs, check_vma=False)
```

```python
import functools

import jax
import jax.numpy as jnp
from jax import lax
from jax.experimental import pallas as pl
from jax.experimental.pallas import tpu as pltpu
from jax.sharding import PartitionSpec as P


ITERS = 3
CODE_STEP = 0.1
EPSILON = 1e-06

D = 64
LANES = 128
F32, BF16 = jnp.float32, jnp.bfloat16
MIB = 1024 * 1024
CHUNK = 256
STEP_VMEM = 52 * MIB
VMEM = pl.BlockSpec(memory_space=pltpu.VMEM)
ANY = pl.BlockSpec(memory_space=pl.ANY)
SMEM = pl.BlockSpec(memory_space=pltpu.SMEM)


def lanes_of(shape):
    return lax.broadcasted_iota(jnp.int32, shape, len(shape) - 1)


def split3(x):
    a = x.astype(BF16).astype(F32)
    rest = x - a
    b = rest.astype(BF16).astype(F32)
    return a, b, rest - b


def operand(y, lane, column):
    left = lane < D
    hi = y.astype(BF16).astype(F32)
    lo = (y - hi).astype(BF16).astype(F32)
    square = (hi + lo) * (hi + lo)
    hi_other, lo_other = pltpu.roll(hi, D, 1), pltpu.roll(lo, D, 1)
    halves = []
    for half in range(2):
        norm = jnp.sum(jnp.where(left == (half == 0), square, 0.0), axis=1, keepdims=True)
        if column:
            norm = norm + EPSILON
        a, b, c = split3(jnp.broadcast_to(norm, y.shape))
        h = (hi, hi_other)[half]
        if column:
            extra = jnp.where(lane == 69, c, 0.0)
            extra = jnp.where(lane == 68, b, extra)
            extra = jnp.where(lane == 67, a, extra)
            extra = jnp.where(lane < 67, 1.0, extra)
            first = -2.0 * jnp.where(left, h, (lo_other, lo)[half])
            second = jnp.where(left, -2.0 * h, extra)
        else:
            extra = jnp.where(lane < 70, 1.0, 0.0)
            extra = jnp.where(lane == 66, c, extra)
            extra = jnp.where(lane == 65, b, extra)
            extra = jnp.where(lane == 64, a, extra)
            first = jnp.where(left, h, (hi_other, hi)[half])
            second = jnp.where(left, (lo, lo_other)[half], extra)
        halves.append((first.astype(BF16), second.astype(BF16)))
    return halves


def convert(place, rows, code_buf, class_buf, pair_buf):
    slab = pair_buf.shape[2]
    per_row = slab // LANES

    def sixteen(k, _):
        top = pl.multiple_of(rows[0] + k * 16, 16)
        for c in range(per_row):
            weight, code = [], []
            for g in (0, 8):
                where = pl.ds((top + g) * per_row + c, 8, stride=per_row)
                kind = class_buf[where, :]
                w = jnp.where(kind == 0, 12.0, jnp.where(kind == 1, 6.0, jnp.where(kind == 2, 4.0, 3.0)))
                weight.append(w)
                code.append((code_buf[where, :] + 1).astype(F32))
            cols = slice(c * LANES, (c + 1) * LANES)
            pair_buf[0, pl.ds(top, 16), cols] = jnp.concatenate(weight, axis=0).astype(BF16)
            pair_buf[1, pl.ds(top, 16), cols] = jnp.concatenate(code, axis=0).astype(BF16)
        return 0

    lax.fori_loop(0, (rows[1] - rows[0]) // 16, sixteen, 0)

    @pl.when((place[1] * D >= rows[0]) & (place[1] * D < rows[1]))
    def _():
        top = pl.multiple_of(place[1] * D, D)
        side = pl.multiple_of(place[0] // 2 * LANES, LANES)
        shape = (D, LANES)
        own = lax.broadcasted_iota(jnp.int32, shape, 0) == lanes_of(shape) - place[0] % 2 * D
        w = pair_buf[0, pl.ds(top, D), pl.ds(side, LANES)].astype(F32)
        pair_buf[0, pl.ds(top, D), pl.ds(side, LANES)] = jnp.where(own, 0.0, w).astype(BF16)


def step_kernel(first, order, place, rows_ref, near_ref, far_ref, *refs):
    if first:
        codes, classes, out, pair, left_op, right_op, code_buf, class_buf, pair_buf, in_sems, out_sems = refs
    else:
        pair, out, left_op, right_op, pair_buf, in_sems = refs
    members, packed, _ = rows_ref.shape
    _, band, slab = pair_buf.shape
    per_row = slab // LANES
    chunks = band // CHUNK

    def fetch(c):
        height = CHUNK * per_row if first else CHUNK
        rows = pl.ds(c * height, height)
        if first:
            ends = ((codes.at[rows], code_buf.at[rows]), (classes.at[rows], class_buf.at[rows]))
        else:
            ends = tuple((pair.at[at, rows], pair_buf.at[at, rows]) for at in (0, 1))
        return [pltpu.make_async_copy(src, dst, in_sems.at[at, c]) for at, (src, dst) in enumerate(ends)]

    def store(c):
        rows = pl.ds(c * CHUNK, CHUNK)
        return [pltpu.make_async_copy(pair_buf.at[at, rows], pair.at[at, rows], out_sems.at[at, c]) for at in (0, 1)]

    def start_fetch(c, _):
        for copy in fetch(c):
            copy.start()
        return 0

    lax.fori_loop(0, chunks, start_fetch, 0)

    lane = lanes_of((packed, LANES))
    left = lane < D
    for j, steps in enumerate(order):
        ref, k = (near_ref, j) if j < len(order) // 2 else (far_ref, j - len(order) // 2)
        for half, (one, two) in enumerate(operand(ref[k], lane, True)):
            at = pl.multiple_of((place[0] ^ steps) * D + half * packed, packed)
            right_op[pl.ds(at, packed), :LANES] = one
            right_op[pl.ds(at, packed), LANES:] = two
    for m in range(members):
        for half, (one, two) in enumerate(operand(rows_ref[m], lane, False)):
            at = m * D + half * packed
            left_op[at : at + packed, :LANES] = one
            left_op[at : at + packed, LANES:] = two

    group = lanes_of((8, LANES)) // 16
    for c in range(chunks):
        rows = slice(c * CHUNK, (c + 1) * CHUNK)
        for k in [c] if first else range(chunks) if c == 0 else ():
            for copy in fetch(k):
                copy.wait()
        if first:
            convert(place, (c * CHUNK, (c + 1) * CHUNK), code_buf, class_buf, pair_buf)
            for copy in store(c):
                copy.start()
            sums = jnp.dot(pair_buf[0, rows, :], jnp.ones((slab, LANES), BF16), preferred_element_type=F32)
        a = left_op[rows, :]
        acc = jnp.zeros((CHUNK, 2 * LANES), F32)
        for n in range(slab // 256):
            cols = slice(n * 256, (n + 1) * 256)
            b = right_op[cols, :]
            dist_sq = lax.dot_general(a, b, (((1,), (1,)), ((), ())), preferred_element_type=F32)
            near = lax.rsqrt(jnp.maximum(dist_sq, EPSILON))
            gap = pair_buf[0, rows, cols].astype(F32) * (1.0 / CODE_STEP - pair_buf[1, rows, cols].astype(F32) * near)
            acc = acc + jnp.dot(gap.astype(BF16), b, preferred_element_type=F32)
        pulled = acc[:, :LANES]
        pulled = -0.5 * (pulled + pltpu.roll(pulled, D, 1))
        total = jnp.broadcast_to(acc[:, LANES + D : LANES + D + 1], (CHUNK, LANES))
        for k in range(CHUNK // D):
            m = c * (CHUNK // D) + k
            y = rows_ref[m]
            lower = slice(k * D, k * D + packed)
            upper = slice(k * D + packed, (k + 1) * D)
            out[m, :packed, :] = jnp.where(left, pulled[lower] - y * total[lower], pulled[upper] - y * total[upper])
            if first:
                tile = jnp.zeros((8, LANES), F32)
                for g in range(D // 8):
                    tile = jnp.where(group == g, sums[k * D + g * 8 : k * D + g * 8 + 8], tile)
                out[m, packed:, :] = tile
    if first:
        for c in range(chunks):
            for copy in store(c):
                copy.wait()


def step(place, rows, columns, *sources):
    members, packed, _ = rows.shape
    near, far, order = columns
    first = len(sources) == 2
    band = members * 2 * packed
    slab = len(order) * 2 * packed
    pair = (2, band, slab)
    outs = [jax.ShapeDtypeStruct((members, packed + (8 if first else 0), LANES), F32)]
    scratch = [pltpu.VMEM((band, 2 * LANES), BF16), pltpu.VMEM((slab, 2 * LANES), BF16)]
    sems = pltpu.SemaphoreType.DMA((2, band // CHUNK))
    if first:
        flat = (band * slab // LANES, LANES)
        sources = tuple(source.reshape(flat) for source in sources)
        outs.append(jax.ShapeDtypeStruct(pair, BF16))
        scratch += [pltpu.VMEM(flat, jnp.int32), pltpu.VMEM(flat, jnp.int32), pltpu.VMEM(pair, BF16), sems, sems]
    else:
        scratch += [pltpu.VMEM(pair, BF16), sems]
    return pl.pallas_call(
        functools.partial(step_kernel, first, order),
        out_shape=tuple(outs),
        in_specs=[SMEM] + [VMEM] * 3 + [ANY] * len(sources),
        out_specs=(VMEM, ANY) if first else (VMEM,),
        scratch_shapes=scratch,
        name="step",
        compiler_params=pltpu.CompilerParams(vmem_limit_bytes=STEP_VMEM),
        cost_estimate=pl.CostEstimate(flops=2 * 10**9, bytes_accessed=5 * MIB, transcendentals=MIB),
    )(place, rows, near, far, *sources)


def sum_of(parts):
    return functools.reduce(jnp.add, [parts[m] for m in range(parts.shape[0])])


def update_kernel(first, last, parts, own, scale, *outs):
    packed = own.shape[0]
    lane = lanes_of((packed, LANES))
    left = lane < D
    if first:
        tile = sum_of(parts.at[:, packed:, :])
        halves = []
        for half in range(2):
            groups = [half * 4 + k for k in range(packed // 8)]
            halves.append(jnp.concatenate([jnp.broadcast_to(tile[:, g * 16 : g * 16 + 1], (8, LANES)) for g in groups], axis=0))
        inverse = CODE_STEP / jnp.where(left, halves[0], halves[1])
        outs[-1][...] = inverse
    else:
        inverse = scale[...]
    moved = own[...] + sum_of(parts.at[:, :packed, :]) * inverse
    if last:
        outs[0][:packed, :] = moved[:, :D]
        outs[0][packed:, :] = pltpu.roll(moved, D, 1)[:, :D]
    else:
        outs[0][...] = moved


def update(parts, own, scale, first, last):
    packed = own.shape[0]
    shape = jax.ShapeDtypeStruct((2 * packed, D) if last else own.shape, F32)
    outs = (shape, jax.ShapeDtypeStruct(own.shape, F32)) if first else (shape,)
    return pl.pallas_call(
        functools.partial(update_kernel, first, last),
        out_shape=outs,
        in_specs=[VMEM] * 3,
        out_specs=(VMEM,) * len(outs),
        name="update",
        compiler_params=pltpu.CompilerParams(vmem_limit_bytes=4 * MIB),
    )(parts, own, scale)


def exchange(parts, axis):
    return lax.all_to_all(parts, axis, split_axis=0, concat_axis=0, tiled=True)


def swapped(value, steps):
    return lax.ppermute(value, "blk", [(at, at ^ steps) for at in range(lax.axis_size("blk"))])


def column_blocks(own):
    block = own[None]
    held = jnp.concatenate([block, swapped(block, 8)])
    near = jnp.concatenate([held, swapped(held, 2), swapped(held, 6), swapped(held, 4)])
    order = [a ^ b for a in (0, 2, 6, 4) for b in (0, 8)]
    return near, swapped(near, 1), order + [a ^ 1 for a in order]


def body(coords, codes, classes):
    packed = coords.shape[0] // 2
    members = lax.axis_size("member")
    place = jnp.stack([lax.axis_index("blk"), lax.axis_index("member")]).astype(jnp.int32)
    own = jnp.concatenate([coords[:packed], coords[packed:]], axis=1)
    scale = own
    sources = (codes, classes)
    for at in range(ITERS):
        rows = exchange(jnp.broadcast_to(own, (members, *own.shape)), "member")
        parts, *pair = step(place, rows, column_blocks(own), *sources)
        if at == 0:
            sources = pair
        outs = update(exchange(parts, "member"), own, scale, at == 0, at == ITERS - 1)
        own = outs[0]
        if at == 0:
            scale = outs[1]
    return own


def solution(mesh):
    in_specs = (P(("blk", "member"), None), P("blk", "member", None), P("blk", "member", None))
    out_specs = P(("blk", "member"), None)
    return jax.shard_map(body, mesh=mesh, in_specs=in_specs, out_specs=out_specs, check_vma=False)
```
